32 devices in a mesh: row: 4 (over y, x), col: 8 (over z, core).
Axes of the slice: x: 2, y: 2, z: 4, core: 2. Of those that a mesh axis runs over, the one named last changes fastest.
Arguments:
- initial_field: float32 [256, 256, 256], P(('row', 'col')), may hold values from -5 to 5
Outputs:
- advanced_field: float32 [256, 256, 256], P(('row', 'col'))
The draws below stay inside these ranges and needn't reach their ends.
All inputs are finite; a program needn't handle non-finite values.
Results may differ from the reference program's by a relative error of at most 0.0003.
Values sent between devices are 32-bit elements; how exact they have to be, the bound alone decides.
A program may use at most 128 MiB of HBM per device.

```python
import math
import jax
import jax.numpy as jnp

NX = 256
NY = 256
NZ = 256


def level_of(stream_key, dims, split, least, high):
    def one(position, blocks):
        heights = jax.random.uniform(jax.random.fold_in(jax.random.fold_in(stream_key, 6), position), (blocks,), jnp.float32, least / len(split), high / len(split))
        return jnp.repeat(jnp.exp(heights), dims[position] // blocks).reshape((-1,) + (1,) * (len(dims) - position - 1))

    gain = one(*split[0])
    for cut in split[1:]:
        gain = gain * one(*cut)
    return gain


def noise(own_key, dims, scale, bound, split=(), dtype=jnp.bfloat16):
    result = scale * jax.random.normal(own_key, dims, jnp.float32)
    if split:
        result = result * level_of(own_key, dims, split, -0.22, 0.18)
    return jnp.clip(result, -bound, bound).astype(dtype)


def setup_inputs(seed: int = 0) -> dict:
    key_of = jax.random.split(jax.random.key(seed), 2)
    initial_field = noise(key_of[0], (NX, NY, NZ), 1.0, 5.0, ((0, 32),), jnp.float32)
    return dict(initial_field=initial_field)


growth_rate = 0.3
quadratic = 1.0
time_step = 0.2
wave_scale = 4.0


def wavenumbers(count, offset, length):
    indices = (offset + jnp.arange(count)).astype(jnp.int32)
    signed = jnp.where(indices * 2 < length, indices, indices - length)
    return wave_scale * signed.astype(jnp.float32) / length


def phi_values(argument):
    within = jnp.abs(argument) < 1.0
    inside = jnp.where(within, argument, 0.0)
    outside = jnp.where(within, 2.0, argument)
    series = []
    for degree in (1, 2, 3):
        running = jnp.zeros_like(argument) + 1.0 / math.factorial(11 + degree)
        for exponent in range(10, -1, -1):
            running = running * inside + 1.0 / math.factorial(exponent + degree)
        series.append(running)
    growth_term = jnp.exp(outside)
    closed_one = (growth_term - 1.0) / outside
    closed_two = (growth_term - 1.0 - outside) / (outside * outside)
    closed_three = (growth_term - 1.0 - outside - 0.5 * outside * outside) / (outside * outside * outside)
    return (jnp.where(within, series[0], closed_one), jnp.where(within, series[1], closed_two), jnp.where(within, series[2], closed_three))


def step_factors(ksq):
    lin = growth_rate - (1.0 - ksq) * (1.0 - ksq)
    scaled = time_step * lin
    half_phi, _, _ = phi_values(0.5 * scaled)
    first_phi, second_phi, third_phi = phi_values(scaled)
    e_half = jnp.exp(0.5 * scaled)
    q_half = 0.5 * time_step * half_phi
    e_full = jnp.exp(scaled)
    f_one = time_step * (first_phi - 3.0 * second_phi + 4.0 * third_phi)
    f_two = time_step * (second_phi - 2.0 * third_phi)
    f_three = time_step * (4.0 * third_phi - second_phi)
    return e_half, q_half, e_full, f_one, f_two, f_three


def reaction(values):
    return quadratic * values * values - values * values * values


def reference(initial_field):
    wave_x = wavenumbers(NX, 0, NX)
    wave_y = wavenumbers(NY, 0, NY)
    wave_z = wavenumbers(NZ, 0, NZ)
    ksq = wave_x[:, None, None] ** 2 + wave_y[None, :, None] ** 2 + wave_z[None, None, :] ** 2
    e_half, q_half, e_full, f_one, f_two, f_three = step_factors(ksq)

    def forward_fft(values):
        return jnp.fft.fftn(values)

    def inverse_fft(spectrum):
        return jnp.fft.ifftn(spectrum).real

    state_hat = forward_fft(initial_field)
    react_u = forward_fft(reaction(initial_field))
    first_hat = e_half * state_hat + q_half * react_u
    react_a = forward_fft(reaction(inverse_fft(first_hat)))
    second_hat = e_half * state_hat + q_half * react_a
    react_b = forward_fft(reaction(inverse_fft(second_hat)))
    third_hat = e_half * first_hat + q_half * (2.0 * react_b - react_u)
    react_c = forward_fft(reaction(inverse_fft(third_hat)))
    new_hat = e_full * state_hat + f_one * react_u + 2.0 * f_two * (react_a + react_b) + f_three * react_c
    return inverse_fft(new_hat).astype(jnp.float32)
```

```python
import functools
import math

import jax
import jax.numpy as jnp
import numpy as np
from jax import lax
from jax.experimental import pallas as pl
from jax.experimental.pallas import tpu as pltpu
from jax.sharding import PartitionSpec as P

growth_rate = 0.3
quadratic = 1.0
time_step = 0.2
wave_scale = 4.0


def wavenumbers(count, offset, length):
    indices = offset + jnp.arange(count)
    signed = jnp.where(indices * 2 < length, indices, indices - length)
    return wave_scale * signed.astype(jnp.float32) / length


def phi_values(argument):
    within = jnp.abs(argument) < 1.0
    inside = jnp.where(within, argument, 0.0)
    outside = jnp.where(within, 2.0, argument)
    series = []
    for degree in (1, 2, 3):
        running = jnp.zeros_like(argument) + 1.0 / math.factorial(11 + degree)
        for exponent in range(10, -1, -1):
            running = running * inside + 1.0 / math.factorial(exponent + degree)
        series.append(running)
    growth_term = jnp.exp(outside)
    closed_one = (growth_term - 1.0) / outside
    closed_two = (growth_term - 1.0 - outside) / (outside * outside)
    closed_three = (growth_term - 1.0 - outside - 0.5 * outside * outside) / (
        outside * outside * outside
    )
    return (
        jnp.where(within, series[0], closed_one),
        jnp.where(within, series[1], closed_two),
        jnp.where(within, series[2], closed_three),
    )


def step_factors(ksq):
    lin = growth_rate - (1.0 - ksq) * (1.0 - ksq)
    scaled = time_step * lin
    half_phi, _, _ = phi_values(0.5 * scaled)
    first_phi, second_phi, third_phi = phi_values(scaled)
    e_half = jnp.exp(0.5 * scaled)
    q_half = 0.5 * time_step * half_phi
    e_full = jnp.exp(scaled)
    f_one = time_step * (first_phi - 3.0 * second_phi + 4.0 * third_phi)
    f_two = time_step * (second_phi - 2.0 * third_phi)
    f_three = time_step * (4.0 * third_phi - second_phi)
    return (e_half, q_half, e_full, f_one, f_two, f_three)


def reaction(values):
    return quadratic * values * values - values * values * values


def cas_table(length):
    modes = jnp.arange(length, dtype=jnp.int32)
    product = jnp.mod(modes[:, None] * modes[None, :], length)
    angle = 2.0 * math.pi / length * product.astype(jnp.float32)
    return (jnp.cos(angle) + jnp.sin(angle)) / math.sqrt(length)


def contract(form, left, right):
    return jnp.einsum(
        form, left, right, precision=lax.Precision.HIGHEST, preferred_element_type=jnp.float32
    )


def move(blocks):
    return lax.all_to_all(blocks, ("row", "col"), split_axis=0, concat_axis=0, tiled=True)


def plain_body(initial_field):
    devices_all = lax.axis_size("row") * lax.axis_size("col")
    rows_x, size_y, size_z = initial_field.shape
    size_x = rows_x * devices_all
    share_y = size_y // devices_all
    table_z = cas_table(size_z)
    table_y = cas_table(size_y).reshape((devices_all, share_y, size_y))
    table_x = cas_table(size_x).reshape((devices_all, rows_x, size_x))
    offset = lax.axis_index(("row", "col")) * share_y
    wave_y = wavenumbers(share_y, offset, size_y)
    wave_z = wavenumbers(size_z, 0, size_z)
    wave_x = wavenumbers(size_x, 0, size_x)
    ksq = wave_y[:, None, None] ** 2 + wave_z[None, None, :] ** 2 + wave_x[None, :, None] ** 2
    e_half, q_half, e_full, f_one, f_two, f_three = step_factors(ksq)

    def forward_all(values):
        over_z = contract("xyn,nk->xyk", values, table_z)
        over_y = contract("sly,xyk->slxk", table_y, over_z)
        return contract("sxX,slxk->lXk", table_x, move(over_y))

    def inverse_all(spectra):
        over_x = contract("sxX,lXk->slxk", table_x, spectra)
        over_y = contract("slxk,sly->xyk", move(over_x), table_y)
        return contract("xyk,kn->xyn", over_y, table_z)

    def react_spectrum(spectrum):
        return forward_all(reaction(inverse_all(spectrum)))

    state_hat = forward_all(initial_field)
    react_u = forward_all(reaction(initial_field))
    first_hat = e_half * state_hat + q_half * react_u
    react_a = react_spectrum(first_hat)
    second_hat = e_half * state_hat + q_half * react_a
    react_b = react_spectrum(second_hat)
    third_hat = e_half * first_hat + q_half * (2.0 * react_b - react_u)
    react_c = react_spectrum(third_hat)
    new_hat = (
        e_full * state_hat + f_one * react_u + 2.0 * f_two * (react_a + react_b) + f_three * react_c
    )
    return inverse_all(new_hat)


LANES = 128


def split_table(length):
    modes = np.arange(length)
    angle = 2.0 * np.pi / length * ((modes[:, None] * modes[None, :]) % length)
    table = ((np.cos(angle) + np.sin(angle)) / np.sqrt(length)).astype(np.float32)
    upper = table.astype(jnp.bfloat16)
    lower = (table - upper.astype(np.float32)).astype(jnp.bfloat16)
    return upper, lower


def split_values(values):
    upper = values.astype(jnp.bfloat16)
    lower = (values - upper.astype(jnp.float32)).astype(jnp.bfloat16)
    return upper, lower


def kernel(
    count, columns, rows_x, share_y, size_x, size_y, size_z,
    field, left, right, out,
    send_f, got_f, send_i, got_i, held, third, total,
    e_half, q_half, e_full, f_one, f_two, f_three,
    sent_f, came_f, sent_i, came_i,
):
    me = lax.axis_index("row") * columns + lax.axis_index("col")
    block = rows_x * share_y
    halves = size_z // LANES
    pairs = share_y // 2
    group = 2 if rows_x % 2 == 0 else 1

    def mul_left(values):
        upper, lower = split_values(values)
        stacked = jnp.concatenate([upper, lower, upper], axis=0)
        return jnp.dot(left[...], stacked, preferred_element_type=jnp.float32)

    def mul_right(values):
        upper, lower = split_values(values)
        stacked = jnp.concatenate([upper, lower, upper], axis=1)
        return jnp.dot(stacked, right[...], preferred_element_type=jnp.float32)

    def send_forward(index, half, start, length):
        buffer = index % 2
        here = pl.multiple_of(me * block + start, 8)
        mine = got_f.at[buffer, half, pl.ds(here, length), :]
        pltpu.make_async_copy(
            send_f.at[buffer, half, me, pl.ds(start, length), :], mine, came_f.at[index, half]
        ).start()

        def one(offset, carry):
            other = (me + offset) % count
            pltpu.make_async_remote_copy(
                src_ref=send_f.at[buffer, half, other, pl.ds(start, length), :],
                dst_ref=mine,
                send_sem=sent_f.at[index, half],
                recv_sem=came_f.at[index, half],
                device_id=(other // columns, other % columns),
                device_id_type=pl.DeviceIdType.MESH,
            ).start()
            return carry

        lax.fori_loop(1, count, one, 0)

    def send_inverse(index, half):
        mine = got_i.at[half, me]

        def rows(device):
            return send_i.at[half, pl.ds(pl.multiple_of(device * block, 8), block), :]

        pltpu.make_async_copy(rows(me), mine, came_i.at[index, half]).start()

        def one(offset, carry):
            other = (me + offset) % count
            pltpu.make_async_remote_copy(
                src_ref=rows(other),
                dst_ref=mine,
                send_sem=sent_i.at[index, half],
                recv_sem=came_i.at[index, half],
                device_id=(other // columns, other % columns),
                device_id_type=pl.DeviceIdType.MESH,
            ).start()
            return carry

        lax.fori_loop(1, count, one, 0)

    def wait_bytes(ref, sem):
        pltpu.make_async_copy(ref, ref, sem).wait()

    def wait_sent_forward(index):
        for half in range(halves):
            wait_bytes(send_f.at[index % 2, half, pl.ds(0, count - 1)], sent_f.at[index, half])

    def wait_sent_inverse(index, half):
        wait_bytes(send_i.at[half, pl.ds(0, (count - 1) * block), :], sent_i.at[index, half])

    def forward(index, source):
        def plane(m):
            spectrum = mul_left(mul_right(source(m)))
            rows = pl.ds(pl.multiple_of(m * share_y, 8), share_y)
            for half in range(halves):
                part = spectrum[:, half * LANES : (half + 1) * LANES]
                send_f[index % 2, half, :, rows, :] = part.reshape(count, share_y, LANES)

        def step(g, carry):
            for inner in range(group):
                plane(g * group + inner)
            send_forward(
                index, 0, pl.multiple_of(g * group * share_y, 8), group * share_y
            )
            return carry

        lax.fori_loop(0, rows_x // group, step, 0)
        for half in range(1, halves):
            send_forward(index, half, 0, block)

    def physical(m):
        rows = pl.ds(pl.multiple_of(m * share_y, 8), share_y)
        parts = [got_i[half, :, rows, :].reshape(size_y, LANES) for half in range(halves)]
        return mul_right(mul_left(jnp.concatenate(parts, axis=1)))

    def spectrum_at(index, half, pair):
        parts = [
            got_f[index % 2, half, pl.ds(pair * 2 + inner, size_x, stride=share_y), :]
            for inner in range(2)
        ]
        return mul_left(jnp.concatenate(parts, axis=1))

    def arrived_forward(index, half):
        wait_bytes(got_f.at[index % 2, half], came_f.at[index, half])

    def inverse(index, source, update):
        for half in range(halves):
            arrived_forward(source, half)
            if index > 0:
                wait_sent_inverse(index - 1, half)

            def step(pair, carry):
                values = mul_left(update(half, pair, spectrum_at(source, half, pair)))
                for inner in range(2):
                    send_i[half, pl.ds(pair * 2 + inner, size_x, stride=share_y), :] = values[
                        :, inner * LANES : (inner + 1) * LANES
                    ]
                return carry

            lax.fori_loop(0, pairs, step, 0)
            send_inverse(index, half)

    def arrived_inverse(index):
        for half in range(halves):
            wait_bytes(got_i.at[half], came_i.at[index, half])

    def wave(indices, length):
        signed = jnp.where(indices * 2 < length, indices, indices - length)
        return wave_scale * signed.astype(jnp.float32) / length

    forward(0, lambda m: field[m])
    forward(1, lambda m: reaction(field[m]))

    rows_step = 32

    def factors(item, carry):
        half = item // (pairs * (size_x // rows_step))
        rest = item % (pairs * (size_x // rows_step))
        pair = rest // (size_x // rows_step)
        start = pl.multiple_of(rest % (size_x // rows_step) * rows_step, 8)
        dims = (rows_step, 2 * LANES)
        lane = lax.broadcasted_iota(jnp.int32, dims, 1)
        second = (lane >= LANES).astype(jnp.int32)
        index_z = lane - second * LANES + half * LANES
        index_y = second + (me * share_y + pair * 2)
        index_x = lax.broadcasted_iota(jnp.int32, dims, 0) + start
        wave_y, wave_z, wave_x = wave(index_y, size_y), wave(index_z, size_z), wave(index_x, size_x)
        ksq = wave_y * wave_y + wave_z * wave_z + wave_x * wave_x
        values = step_factors(ksq)
        where = pl.ds(start, rows_step)
        for ref, value in zip((e_half, q_half, e_full, f_one, f_two, f_three), values):
            ref[half, pair, where, :] = value
        return carry

    lax.fori_loop(0, halves * pairs * (size_x // rows_step), factors, 0)

    for half in range(halves):
        arrived_forward(0, half)

        def keep(pair, carry):
            total[half, pair] = spectrum_at(0, half, pair)
            return carry

        lax.fori_loop(0, pairs, keep, 0)

    def update_first(half, pair, react_u):
        state_hat = total[half, pair]
        base = e_half[half, pair] * state_hat
        gain = q_half[half, pair] * react_u
        first_hat = base + gain
        held[half, pair] = base
        third[half, pair] = e_half[half, pair] * first_hat - gain
        total[half, pair] = e_full[half, pair] * state_hat + f_one[half, pair] * react_u
        return first_hat

    def update_second(half, pair, react_a):
        total[half, pair] = total[half, pair] + 2.0 * f_two[half, pair] * react_a
        return held[half, pair] + q_half[half, pair] * react_a

    def update_third(half, pair, react_b):
        total[half, pair] = total[half, pair] + 2.0 * f_two[half, pair] * react_b
        return third[half, pair] + 2.0 * q_half[half, pair] * react_b

    def update_last(half, pair, react_c):
        return total[half, pair] + f_three[half, pair] * react_c

    updates = (update_first, update_second, update_third, update_last)
    for index, update in enumerate(updates):
        inverse(index, index + 1, update)
        if index < 3:
            wait_sent_forward(index)
            arrived_inverse(index)
            forward(index + 2, lambda m: reaction(physical(m)))
    for index in (3, 4):
        wait_sent_forward(index)
    arrived_inverse(3)

    def finish(m, carry):
        out[m] = physical(m)
        return carry

    lax.fori_loop(0, rows_x, finish, 0)
    for half in range(halves):
        wait_sent_inverse(3, half)


def body(initial_field):
    rows_x, size_y, size_z = initial_field.shape
    columns = lax.axis_size("col")
    count = lax.axis_size("row") * columns
    size_x = rows_x * count
    share_y = size_y // count
    fits = share_y % 8 == 0 and size_z % LANES == 0 and size_x == size_y == size_z
    if not fits:
        return plain_body(initial_field)
    upper, lower = split_table(size_x)
    left = np.concatenate([upper, upper, lower], axis=1)
    right = np.concatenate([upper, upper, lower], axis=0)
    halves, pairs, block = size_z // LANES, share_y // 2, rows_x * share_y
    spectral = pltpu.VMEM((halves, pairs, size_x, 2 * LANES), jnp.float32)
    vmem = pl.BlockSpec(memory_space=pltpu.VMEM)
    return pl.pallas_call(
        functools.partial(
            kernel, count, columns, rows_x, share_y, size_x, size_y, size_z
        ),
        out_shape=jax.ShapeDtypeStruct(initial_field.shape, jnp.float32),
        in_specs=[vmem] * 3,
        out_specs=vmem,
        scratch_shapes=[
            pltpu.VMEM((2, halves, count, block, LANES), jnp.float32),
            pltpu.VMEM((2, halves, count * block, LANES), jnp.float32),
            pltpu.VMEM((halves, count * block, LANES), jnp.float32),
            pltpu.VMEM((halves, count, block, LANES), jnp.float32),
        ]
        + [spectral] * 9
        + [
            pltpu.SemaphoreType.DMA((5, halves)),
            pltpu.SemaphoreType.DMA((5, halves)),
            pltpu.SemaphoreType.DMA((4, halves)),
            pltpu.SemaphoreType.DMA((4, halves)),
        ],
        compiler_params=pltpu.CompilerParams(
            has_side_effects=True, vmem_limit_bytes=60 * 1024 * 1024
        ),
    )(initial_field, jnp.asarray(left), jnp.asarray(right))


def solution(mesh):
    placed = (P(("row", "col"), None, None),)
    return jax.shard_map(
        body, mesh=mesh, in_specs=placed, out_specs=P(("row", "col"), None, None), check_vma=False
    )
```

```python
import functools
import math

import jax
import jax.numpy as jnp
import numpy as np
from jax import lax
from jax.experimental import pallas as pl
from jax.experimental.pallas import tpu as pltpu
from jax.sharding import PartitionSpec as P

growth_rate = 0.3
quadratic = 1.0
time_step = 0.2
wave_scale = 4.0


def wavenumbers(count, offset, length):
    indices = offset + jnp.arange(count)
    signed = jnp.where(indices * 2 < length, indices, indices - length)
    return wave_scale * signed.astype(jnp.float32) / length


def phi_values(argument):
    within = jnp.abs(argument) < 1.0
    inside = jnp.where(within, argument, 0.0)
    outside = jnp.where(within, 2.0, argument)
    series = []
    for degree in (1, 2, 3):
        running = jnp.zeros_like(argument) + 1.0 / math.factorial(11 + degree)
        for exponent in range(10, -1, -1):
            running = running * inside + 1.0 / math.factorial(exponent + degree)
        series.append(running)
    growth_term = jnp.exp(outside)
    closed_one = (growth_term - 1.0) / outside
    closed_two = (growth_term - 1.0 - outside) / (outside * outside)
    closed_three = (growth_term - 1.0 - outside - 0.5 * outside * outside) / (
        outside * outside * outside
    )
    return (
        jnp.where(within, series[0], closed_one),
        jnp.where(within, series[1], closed_two),
        jnp.where(within, series[2], closed_three),
    )


def step_factors(ksq):
    lin = growth_rate - (1.0 - ksq) * (1.0 - ksq)
    scaled = time_step * lin
    half_phi, _, _ = phi_values(0.5 * scaled)
    first_phi, second_phi, third_phi = phi_values(scaled)
    e_half = jnp.exp(0.5 * scaled)
    q_half = 0.5 * time_step * half_phi
    e_full = jnp.exp(scaled)
    f_one = time_step * (first_phi - 3.0 * second_phi + 4.0 * third_phi)
    f_two = time_step * (second_phi - 2.0 * third_phi)
    f_three = time_step * (4.0 * third_phi - second_phi)
    return (e_half, q_half, e_full, f_one, f_two, f_three)


def reaction(values):
    return quadratic * values * values - values * values * values


def cas_table(length):
    modes = jnp.arange(length, dtype=jnp.int32)
    product = jnp.mod(modes[:, None] * modes[None, :], length)
    angle = 2.0 * math.pi / length * product.astype(jnp.float32)
    return (jnp.cos(angle) + jnp.sin(angle)) / math.sqrt(length)


def contract(form, left, right):
    return jnp.einsum(
        form, left, right, precision=lax.Precision.HIGHEST, preferred_element_type=jnp.float32
    )


def move(blocks):
    return lax.all_to_all(blocks, ("row", "col"), split_axis=0, concat_axis=0, tiled=True)


def plain_body(initial_field):
    devices_all = lax.axis_size("row") * lax.axis_size("col")
    rows_x, size_y, size_z = initial_field.shape
    size_x = rows_x * devices_all
    share_y = size_y // devices_all
    table_z = cas_table(size_z)
    table_y = cas_table(size_y).reshape((devices_all, share_y, size_y))
    table_x = cas_table(size_x).reshape((devices_all, rows_x, size_x))
    offset = lax.axis_index(("row", "col")) * share_y
    wave_y = wavenumbers(share_y, offset, size_y)
    wave_z = wavenumbers(size_z, 0, size_z)
    wave_x = wavenumbers(size_x, 0, size_x)
    ksq = wave_y[:, None, None] ** 2 + wave_z[None, None, :] ** 2 + wave_x[None, :, None] ** 2
    e_half, q_half, e_full, f_one, f_two, f_three = step_factors(ksq)

    def forward_all(values):
        over_z = contract("xyn,nk->xyk", values, table_z)
        over_y = contract("sly,xyk->slxk", table_y, over_z)
        return contract("sxX,slxk->lXk", table_x, move(over_y))

    def inverse_all(spectra):
        over_x = contract("sxX,lXk->slxk", table_x, spectra)
        over_y = contract("slxk,sly->xyk", move(over_x), table_y)
        return contract("xyk,kn->xyn", over_y, table_z)

    def react_spectrum(spectrum):
        return forward_all(reaction(inverse_all(spectrum)))

    state_hat = forward_all(initial_field)
    react_u = forward_all(reaction(initial_field))
    first_hat = e_half * state_hat + q_half * react_u
    react_a = react_spectrum(first_hat)
    second_hat = e_half * state_hat + q_half * react_a
    react_b = react_spectrum(second_hat)
    third_hat = e_half * first_hat + q_half * (2.0 * react_b - react_u)
    react_c = react_spectrum(third_hat)
    new_hat = (
        e_full * state_hat + f_one * react_u + 2.0 * f_two * (react_a + react_b) + f_three * react_c
    )
    return inverse_all(new_hat)


LANES = 128


def split_table(length):
    modes = np.arange(length)
    angle = 2.0 * np.pi / length * ((modes[:, None] * modes[None, :]) % length)
    table = ((np.cos(angle) + np.sin(angle)) / np.sqrt(length)).astype(np.float32)
    upper = table.astype(jnp.bfloat16)
    lower = (table - upper.astype(np.float32)).astype(jnp.bfloat16)
    return upper, lower


def split_values(values):
    upper = values.astype(jnp.bfloat16)
    lower = (values - upper.astype(jnp.float32)).astype(jnp.bfloat16)
    return upper, lower


def kernel(
    count, columns, rows_x, share_y, size_x, size_y, size_z,
    field, left, right, out,
    send_f, got_f, send_i, got_i, held, third, total,
    e_half, q_half, e_full, f_one, f_two, f_three,
    sent_f, came_f, sent_i, came_i,
):
    me = lax.axis_index("row") * columns + lax.axis_index("col")
    block = rows_x * share_y
    halves = size_z // LANES
    pairs = share_y // 2
    group = 2 if rows_x % 2 == 0 else 1
    parts = rows_x // group
    early = parts // 2

    def mul_left(values):
        upper, lower = split_values(values)
        stacked = jnp.concatenate([upper, lower, upper], axis=0)
        return jnp.dot(left[...], stacked, preferred_element_type=jnp.float32)

    def mul_right(values):
        upper, lower = split_values(values)
        stacked = jnp.concatenate([upper, lower, upper], axis=1)
        return jnp.dot(stacked, right[...], preferred_element_type=jnp.float32)

    def send_forward(index, half, start, length):
        buffer = index % 2
        here = pl.multiple_of(me * block + start, 8)
        mine = got_f.at[buffer, half, pl.ds(here, length), :]
        pltpu.make_async_copy(
            send_f.at[buffer, half, me, pl.ds(start, length), :], mine, came_f.at[index, half]
        ).start()

        def one(offset, carry):
            other = (me + offset) % count
            pltpu.make_async_remote_copy(
                src_ref=send_f.at[buffer, half, other, pl.ds(start, length), :],
                dst_ref=mine,
                send_sem=sent_f.at[index, half],
                recv_sem=came_f.at[index, half],
                device_id=(other // columns, other % columns),
                device_id_type=pl.DeviceIdType.MESH,
            ).start()
            return carry

        lax.fori_loop(1, count, one, 0)

    def send_inverse(index, half, part):
        length = group * share_y
        mine = got_i.at[half, me, pl.ds(part * length, length), :]

        def rows(device):
            start = pl.multiple_of(device * block + part * length, 8)
            return send_i.at[half, pl.ds(start, length), :]

        pltpu.make_async_copy(rows(me), mine, came_i.at[index, part]).start()

        def one(offset, carry):
            other = (me + offset) % count
            pltpu.make_async_remote_copy(
                src_ref=rows(other),
                dst_ref=mine,
                send_sem=sent_i.at[index, half],
                recv_sem=came_i.at[index, part],
                device_id=(other // columns, other % columns),
                device_id_type=pl.DeviceIdType.MESH,
            ).start()
            return carry

        lax.fori_loop(1, count, one, 0)

    def wait_bytes(ref, sem):
        pltpu.make_async_copy(ref, ref, sem).wait()

    def wait_sent_forward(index):
        for half in range(halves):
            wait_bytes(send_f.at[index % 2, half, pl.ds(0, count - 1)], sent_f.at[index, half])

    def wait_sent_inverse(index, half):
        wait_bytes(send_i.at[half, pl.ds(0, (count - 1) * block), :], sent_i.at[index, half])

    def forward(index, source, before=None):
        def plane(m):
            spectrum = mul_left(mul_right(source(m)))
            rows = pl.ds(pl.multiple_of(m * share_y, 8), share_y)
            for half in range(halves):
                part = spectrum[:, half * LANES : (half + 1) * LANES]
                send_f[index % 2, half, :, rows, :] = part.reshape(count, share_y, LANES)

        def step(g, carry):
            if before is not None:
                before(g)
            for inner in range(group):
                plane(g * group + inner)
            send_forward(
                index, 0, pl.multiple_of(g * group * share_y, 8), group * share_y
            )
            return carry

        lax.fori_loop(0, rows_x // group, step, 0)
        for half in range(1, halves):
            send_forward(index, half, 0, block)

    def physical(m):
        rows = pl.ds(pl.multiple_of(m * share_y, 8), share_y)
        parts = [got_i[half, :, rows, :].reshape(size_y, LANES) for half in range(halves)]
        return mul_right(mul_left(jnp.concatenate(parts, axis=1)))

    def spectrum_at(index, half, pair):
        parts = [
            got_f[index % 2, half, pl.ds(pair * 2 + inner, size_x, stride=share_y), :]
            for inner in range(2)
        ]
        return mul_left(jnp.concatenate(parts, axis=1))

    def arrived_forward(index, half):
        wait_bytes(got_f.at[index % 2, half], came_f.at[index, half])

    def inverse(index, source, update):
        for half in range(halves):
            arrived_forward(source, half)
            if index > 0:
                wait_sent_inverse(index - 1, half)

            def step(pair, carry):
                values = mul_left(update(half, pair, spectrum_at(source, half, pair)))
                for inner in range(2):
                    send_i[half, pl.ds(pair * 2 + inner, size_x, stride=share_y), :] = values[
                        :, inner * LANES : (inner + 1) * LANES
                    ]
                return carry

            lax.fori_loop(0, pairs, step, 0)
            for part in range(early):
                send_inverse(index, half, part)
        for part in range(early, parts):
            for half in range(halves):
                send_inverse(index, half, part)

    def arrived_inverse(index, part):
        length = group * share_y
        rows = pl.ds(pl.multiple_of(part * length, 8), length)
        wait_bytes(got_i.at[:, :, rows, :], came_i.at[index, part])

    def wave(indices, length):
        signed = jnp.where(indices * 2 < length, indices, indices - length)
        return wave_scale * signed.astype(jnp.float32) / length

    forward(0, lambda m: field[m])
    forward(1, lambda m: reaction(field[m]))

    rows_step = 32

    def factors(item, carry):
        half = item // (pairs * (size_x // rows_step))
        rest = item % (pairs * (size_x // rows_step))
        pair = rest // (size_x // rows_step)
        start = pl.multiple_of(rest % (size_x // rows_step) * rows_step, 8)
        dims = (rows_step, 2 * LANES)
        lane = lax.broadcasted_iota(jnp.int32, dims, 1)
        second = (lane >= LANES).astype(jnp.int32)
        index_z = lane - second * LANES + half * LANES
        index_y = second + (me * share_y + pair * 2)
        index_x = lax.broadcasted_iota(jnp.int32, dims, 0) + start
        wave_y, wave_z, wave_x = wave(index_y, size_y), wave(index_z, size_z), wave(index_x, size_x)
        ksq = wave_y * wave_y + wave_z * wave_z + wave_x * wave_x
        values = step_factors(ksq)
        where = pl.ds(start, rows_step)
        for ref, value in zip((e_half, q_half, e_full, f_one, f_two, f_three), values):
            ref[half, pair, where, :] = value
        return carry

    lax.fori_loop(0, halves * pairs * (size_x // rows_step), factors, 0)

    for half in range(halves):
        arrived_forward(0, half)

        def keep(pair, carry):
            total[half, pair] = spectrum_at(0, half, pair)
            return carry

        lax.fori_loop(0, pairs, keep, 0)

    def update_first(half, pair, react_u):
        state_hat = total[half, pair]
        base = e_half[half, pair] * state_hat
        gain = q_half[half, pair] * react_u
        first_hat = base + gain
        held[half, pair] = base
        third[half, pair] = e_half[half, pair] * first_hat - gain
        total[half, pair] = e_full[half, pair] * state_hat + f_one[half, pair] * react_u
        return first_hat

    def update_second(half, pair, react_a):
        total[half, pair] = total[half, pair] + 2.0 * f_two[half, pair] * react_a
        return held[half, pair] + q_half[half, pair] * react_a

    def update_third(half, pair, react_b):
        total[half, pair] = total[half, pair] + 2.0 * f_two[half, pair] * react_b
        return third[half, pair] + 2.0 * q_half[half, pair] * react_b

    def update_last(half, pair, react_c):
        return total[half, pair] + f_three[half, pair] * react_c

    updates = (update_first, update_second, update_third, update_last)
    for index, update in enumerate(updates):
        inverse(index, index + 1, update)
        if index < 3:
            wait_sent_forward(index)
            forward(
                index + 2,
                lambda m: reaction(physical(m)),
                lambda g, index=index: arrived_inverse(index, g),
            )
    for index in (3, 4):
        wait_sent_forward(index)

    def finish(g, carry):
        arrived_inverse(3, g)
        for inner in range(group):
            out[g * group + inner] = physical(g * group + inner)
        return carry

    lax.fori_loop(0, parts, finish, 0)
    for half in range(halves):
        wait_sent_inverse(3, half)


def body(initial_field):
    rows_x, size_y, size_z = initial_field.shape
    columns = lax.axis_size("col")
    count = lax.axis_size("row") * columns
    size_x = rows_x * count
    share_y = size_y // count
    fits = share_y % 8 == 0 and size_z % LANES == 0 and size_x == size_y == size_z
    if not fits:
        return plain_body(initial_field)
    upper, lower = split_table(size_x)
    left = np.concatenate([upper, upper, lower], axis=1)
    right = np.concatenate([upper, upper, lower], axis=0)
    halves, pairs, block = size_z // LANES, share_y // 2, rows_x * share_y
    spectral = pltpu.VMEM((halves, pairs, size_x, 2 * LANES), jnp.float32)
    vmem = pl.BlockSpec(memory_space=pltpu.VMEM)
    return pl.pallas_call(
        functools.partial(
            kernel, count, columns, rows_x, share_y, size_x, size_y, size_z
        ),
        out_shape=jax.ShapeDtypeStruct(initial_field.shape, jnp.float32),
        in_specs=[vmem] * 3,
        out_specs=vmem,
        scratch_shapes=[
            pltpu.VMEM((2, halves, count, block, LANES), jnp.float32),
            pltpu.VMEM((2, halves, count * block, LANES), jnp.float32),
            pltpu.VMEM((halves, count * block, LANES), jnp.float32),
            pltpu.VMEM((halves, count, block, LANES), jnp.float32),
        ]
        + [spectral] * 9
        + [
            pltpu.SemaphoreType.DMA((5, halves)),
            pltpu.SemaphoreType.DMA((5, halves)),
            pltpu.SemaphoreType.DMA((4, halves)),
            pltpu.SemaphoreType.DMA((4, rows_x)),
        ],
        compiler_params=pltpu.CompilerParams(
            has_side_effects=True, vmem_limit_bytes=60 * 1024 * 1024
        ),
    )(initial_field, jnp.asarray(left), jnp.asarray(right))


def solution(mesh):
    placed = (P(("row", "col"), None, None),)
    return jax.shard_map(
        body, mesh=mesh, in_specs=placed, out_specs=P(("row", "col"), None, None), check_vma=False
    )
```

```python
import functools
import math

import jax
import jax.numpy as jnp
import numpy as np
from jax import lax
from jax.experimental import pallas as pl
from jax.experimental.pallas import tpu as pltpu
from jax.sharding import PartitionSpec as P

growth_rate = 0.3
quadratic = 1.0
time_step = 0.2
wave_scale = 4.0


def wavenumbers(count, offset, length):
    indices = offset + jnp.arange(count)
    signed = jnp.where(indices * 2 < length, indices, indices - length)
    return wave_scale * signed.astype(jnp.float32) / length


def phi_values(argument):
    within = jnp.abs(argument) < 1.0
    inside = jnp.where(within, argument, 0.0)
    outside = jnp.where(within, 2.0, argument)
    series = []
    for degree in (1, 2, 3):
        running = jnp.zeros_like(argument) + 1.0 / math.factorial(11 + degree)
        for exponent in range(10, -1, -1):
            running = running * inside + 1.0 / math.factorial(exponent + degree)
        series.append(running)
    growth_term = jnp.exp(outside)
    closed_one = (growth_term - 1.0) / outside
    closed_two = (growth_term - 1.0 - outside) / (outside * outside)
    closed_three = (growth_term - 1.0 - outside - 0.5 * outside * outside) / (
        outside * outside * outside
    )
    return (
        jnp.where(within, series[0], closed_one),
        jnp.where(within, series[1], closed_two),
        jnp.where(within, series[2], closed_three),
    )


def step_factors(ksq):
    lin = growth_rate - (1.0 - ksq) * (1.0 - ksq)
    scaled = time_step * lin
    half_phi, _, _ = phi_values(0.5 * scaled)
    first_phi, second_phi, third_phi = phi_values(scaled)
    e_half = jnp.exp(0.5 * scaled)
    q_half = 0.5 * time_step * half_phi
    e_full = jnp.exp(scaled)
    f_one = time_step * (first_phi - 3.0 * second_phi + 4.0 * third_phi)
    f_two = time_step * (second_phi - 2.0 * third_phi)
    f_three = time_step * (4.0 * third_phi - second_phi)
    return (e_half, q_half, e_full, f_one, f_two, f_three)


def reaction(values):
    return quadratic * values * values - values * values * values


def cas_table(length):
    modes = jnp.arange(length, dtype=jnp.int32)
    product = jnp.mod(modes[:, None] * modes[None, :], length)
    angle = 2.0 * math.pi / length * product.astype(jnp.float32)
    return (jnp.cos(angle) + jnp.sin(angle)) / math.sqrt(length)


def contract(form, left, right):
    return jnp.einsum(
        form, left, right, precision=lax.Precision.HIGHEST, preferred_element_type=jnp.float32
    )


def move(blocks):
    return lax.all_to_all(blocks, ("row", "col"), split_axis=0, concat_axis=0, tiled=True)


def plain_body(initial_field):
    devices_all = lax.axis_size("row") * lax.axis_size("col")
    rows_x, size_y, size_z = initial_field.shape
    size_x = rows_x * devices_all
    share_y = size_y // devices_all
    table_z = cas_table(size_z)
    table_y = cas_table(size_y).reshape((devices_all, share_y, size_y))
    table_x = cas_table(size_x).reshape((devices_all, rows_x, size_x))
    offset = lax.axis_index(("row", "col")) * share_y
    wave_y = wavenumbers(share_y, offset, size_y)
    wave_z = wavenumbers(size_z, 0, size_z)
    wave_x = wavenumbers(size_x, 0, size_x)
    ksq = wave_y[:, None, None] ** 2 + wave_z[None, None, :] ** 2 + wave_x[None, :, None] ** 2
    e_half, q_half, e_full, f_one, f_two, f_three = step_factors(ksq)

    def forward_all(values):
        over_z = contract("xyn,nk->xyk", values, table_z)
        over_y = contract("sly,xyk->slxk", table_y, over_z)
        return contract("sxX,slxk->lXk", table_x, move(over_y))

    def inverse_all(spectra):
        over_x = contract("sxX,lXk->slxk", table_x, spectra)
        over_y = contract("slxk,sly->xyk", move(over_x), table_y)
        return contract("xyk,kn->xyn", over_y, table_z)

    def react_spectrum(spectrum):
        return forward_all(reaction(inverse_all(spectrum)))

    state_hat = forward_all(initial_field)
    react_u = forward_all(reaction(initial_field))
    first_hat = e_half * state_hat + q_half * react_u
    react_a = react_spectrum(first_hat)
    second_hat = e_half * state_hat + q_half * react_a
    react_b = react_spectrum(second_hat)
    third_hat = e_half * first_hat + q_half * (2.0 * react_b - react_u)
    react_c = react_spectrum(third_hat)
    new_hat = (
        e_full * state_hat + f_one * react_u + 2.0 * f_two * (react_a + react_b) + f_three * react_c
    )
    return inverse_all(new_hat)


LANES = 128


def split_table(length):
    modes = np.arange(length)
    angle = 2.0 * np.pi / length * ((modes[:, None] * modes[None, :]) % length)
    table = ((np.cos(angle) + np.sin(angle)) / np.sqrt(length)).astype(np.float32)
    upper = table.astype(jnp.bfloat16)
    lower = (table - upper.astype(np.float32)).astype(jnp.bfloat16)
    return upper, lower


def split_values(values):
    upper = values.astype(jnp.bfloat16)
    lower = (values - upper.astype(jnp.float32)).astype(jnp.bfloat16)
    return upper, lower


def kernel(
    count, columns, rows_x, share_y, size_x, size_y, size_z,
    field, left, right, out,
    send_f, got_f, send_i, got_i, held, third, total,
    e_half, q_half, e_full, f_one, f_two, f_three,
    sent_f, came_f, sent_i, came_i,
):
    me = lax.axis_index("row") * columns + lax.axis_index("col")
    block = rows_x * share_y
    halves = size_z // LANES
    pairs = share_y // 2
    group = 2 if rows_x % 2 == 0 else 1
    parts = rows_x // group
    early = parts // 2

    def mul_left(values):
        upper, lower = split_values(values)
        stacked = jnp.concatenate([upper, lower, upper], axis=0)
        return jnp.dot(left[...], stacked, preferred_element_type=jnp.float32)

    def mul_right(values):
        upper, lower = split_values(values)
        stacked = jnp.concatenate([upper, lower, upper], axis=1)
        return jnp.dot(stacked, right[...], preferred_element_type=jnp.float32)

    barrier = pltpu.get_barrier_semaphore()

    def greet(offset, carry):
        other = (me + offset) % count
        pl.semaphore_signal(
            barrier,
            inc=1,
            device_id=(other // columns, other % columns),
            device_id_type=pl.DeviceIdType.MESH,
        )
        return carry

    lax.fori_loop(1, count, greet, 0)

    def send_forward(index, half, start, length):
        buffer = index % 2
        here = pl.multiple_of(me * block + start, 8)
        mine = got_f.at[buffer, half, pl.ds(here, length), :]
        pltpu.make_async_copy(
            send_f.at[buffer, half, me, pl.ds(start, length), :], mine, came_f.at[index, half]
        ).start()

        def one(offset, carry):
            other = (me + offset) % count
            pltpu.make_async_remote_copy(
                src_ref=send_f.at[buffer, half, other, pl.ds(start, length), :],
                dst_ref=mine,
                send_sem=sent_f.at[index, half],
                recv_sem=came_f.at[index, half],
                device_id=(other // columns, other % columns),
                device_id_type=pl.DeviceIdType.MESH,
            ).start()
            return carry

        lax.fori_loop(1, count, one, 0)

    def send_inverse(index, half, part):
        length = group * share_y
        mine = got_i.at[half, me, pl.ds(part * length, length), :]

        def rows(device):
            start = pl.multiple_of(device * block + part * length, 8)
            return send_i.at[half, pl.ds(start, length), :]

        pltpu.make_async_copy(rows(me), mine, came_i.at[index, part]).start()

        def one(offset, carry):
            other = (me + offset) % count
            pltpu.make_async_remote_copy(
                src_ref=rows(other),
                dst_ref=mine,
                send_sem=sent_i.at[index, half],
                recv_sem=came_i.at[index, part],
                device_id=(other // columns, other % columns),
                device_id_type=pl.DeviceIdType.MESH,
            ).start()
            return carry

        lax.fori_loop(1, count, one, 0)

    def wait_bytes(ref, sem):
        pltpu.make_async_copy(ref, ref, sem).wait()

    def wait_sent_forward(index):
        for half in range(halves):
            wait_bytes(send_f.at[index % 2, half, pl.ds(0, count - 1)], sent_f.at[index, half])

    def wait_sent_inverse(index, half):
        wait_bytes(send_i.at[half, pl.ds(0, (count - 1) * block), :], sent_i.at[index, half])

    def forward(index, source, before=None):
        def plane(m):
            spectrum = mul_left(mul_right(source(m)))
            rows = pl.ds(pl.multiple_of(m * share_y, 8), share_y)
            for half in range(halves):
                part = spectrum[:, half * LANES : (half + 1) * LANES]
                send_f[index % 2, half, :, rows, :] = part.reshape(count, share_y, LANES)

        def step(g, carry):
            if before is not None:
                before(g)
            for inner in range(group):
                plane(g * group + inner)
            send_forward(
                index, 0, pl.multiple_of(g * group * share_y, 8), group * share_y
            )
            return carry

        first = 0
        if index == 0:
            for m in range(group):
                plane(m)
            pl.semaphore_wait(barrier, count - 1)
            send_forward(0, 0, 0, group * share_y)
            first = 1
        lax.fori_loop(first, parts, step, 0)
        for half in range(1, halves):
            send_forward(index, half, 0, block)

    def physical(m):
        rows = pl.ds(pl.multiple_of(m * share_y, 8), share_y)
        parts = [got_i[half, :, rows, :].reshape(size_y, LANES) for half in range(halves)]
        return mul_right(mul_left(jnp.concatenate(parts, axis=1)))

    def spectrum_at(index, half, pair):
        parts = [
            got_f[index % 2, half, pl.ds(pair * 2 + inner, size_x, stride=share_y), :]
            for inner in range(2)
        ]
        return mul_left(jnp.concatenate(parts, axis=1))

    def arrived_forward(index, half):
        wait_bytes(got_f.at[index % 2, half], came_f.at[index, half])

    def inverse(index, source, update):
        for half in range(halves):
            arrived_forward(source, half)
            if index > 0:
                wait_sent_inverse(index - 1, half)

            def step(pair, carry):
                values = mul_left(update(half, pair, spectrum_at(source, half, pair)))
                for inner in range(2):
                    send_i[half, pl.ds(pair * 2 + inner, size_x, stride=share_y), :] = values[
                        :, inner * LANES : (inner + 1) * LANES
                    ]
                return carry

            lax.fori_loop(0, pairs, step, 0)
            for part in range(early):
                send_inverse(index, half, part)
        for part in range(early, parts):
            for half in range(halves):
                send_inverse(index, half, part)

    def arrived_inverse(index, part):
        length = group * share_y
        rows = pl.ds(pl.multiple_of(part * length, 8), length)
        wait_bytes(got_i.at[:, :, rows, :], came_i.at[index, part])

    def wave(indices, length):
        signed = jnp.where(indices * 2 < length, indices, indices - length)
        return wave_scale * signed.astype(jnp.float32) / length

    forward(0, lambda m: field[m])
    forward(1, lambda m: reaction(field[m]))

    rows_step = 32

    def factors(item, carry):
        half = item // (pairs * (size_x // rows_step))
        rest = item % (pairs * (size_x // rows_step))
        pair = rest // (size_x // rows_step)
        start = pl.multiple_of(rest % (size_x // rows_step) * rows_step, 8)
        dims = (rows_step, 2 * LANES)
        lane = lax.broadcasted_iota(jnp.int32, dims, 1)
        second = (lane >= LANES).astype(jnp.int32)
        index_z = lane - second * LANES + half * LANES
        index_y = second + (me * share_y + pair * 2)
        index_x = lax.broadcasted_iota(jnp.int32, dims, 0) + start
        wave_y, wave_z, wave_x = wave(index_y, size_y), wave(index_z, size_z), wave(index_x, size_x)
        ksq = wave_y * wave_y + wave_z * wave_z + wave_x * wave_x
        values = step_factors(ksq)
        where = pl.ds(start, rows_step)
        for ref, value in zip((e_half, q_half, e_full, f_one, f_two, f_three), values):
            ref[half, pair, where, :] = value
        return carry

    lax.fori_loop(0, halves * pairs * (size_x // rows_step), factors, 0)

    for half in range(halves):
        arrived_forward(0, half)

        def keep(pair, carry):
            total[half, pair] = spectrum_at(0, half, pair)
            return carry

        lax.fori_loop(0, pairs, keep, 0)

    def update_first(half, pair, react_u):
        state_hat = total[half, pair]
        base = e_half[half, pair] * state_hat
        gain = q_half[half, pair] * react_u
        first_hat = base + gain
        held[half, pair] = base
        third[half, pair] = e_half[half, pair] * first_hat - gain
        total[half, pair] = e_full[half, pair] * state_hat + f_one[half, pair] * react_u
        return first_hat

    def update_second(half, pair, react_a):
        total[half, pair] = total[half, pair] + 2.0 * f_two[half, pair] * react_a
        return held[half, pair] + q_half[half, pair] * react_a

    def update_third(half, pair, react_b):
        total[half, pair] = total[half, pair] + 2.0 * f_two[half, pair] * react_b
        return third[half, pair] + 2.0 * q_half[half, pair] * react_b

    def update_last(half, pair, react_c):
        return total[half, pair] + f_three[half, pair] * react_c

    updates = (update_first, update_second, update_third, update_last)
    for index, update in enumerate(updates):
        inverse(index, index + 1, update)
        if index < 3:
            wait_sent_forward(index)
            forward(
                index + 2,
                lambda m: reaction(physical(m)),
                lambda g, index=index: arrived_inverse(index, g),
            )
    for index in (3, 4):
        wait_sent_forward(index)

    def finish(g, carry):
        arrived_inverse(3, g)
        for inner in range(group):
            out[g * group + inner] = physical(g * group + inner)
        return carry

    lax.fori_loop(0, parts, finish, 0)
    for half in range(halves):
        wait_sent_inverse(3, half)


def body(initial_field):
    rows_x, size_y, size_z = initial_field.shape
    columns = lax.axis_size("col")
    count = lax.axis_size("row") * columns
    size_x = rows_x * count
    share_y = size_y // count
    fits = share_y % 8 == 0 and size_z % LANES == 0 and size_x == size_y == size_z
    if not fits:
        return plain_body(initial_field)
    upper, lower = split_table(size_x)
    left = np.concatenate([upper, upper, lower], axis=1)
    right = np.concatenate([upper, upper, lower], axis=0)
    halves, pairs, block = size_z // LANES, share_y // 2, rows_x * share_y
    spectral = pltpu.VMEM((halves, pairs, size_x, 2 * LANES), jnp.float32)
    vmem = pl.BlockSpec(memory_space=pltpu.VMEM)
    return pl.pallas_call(
        functools.partial(
            kernel, count, columns, rows_x, share_y, size_x, size_y, size_z
        ),
        out_shape=jax.ShapeDtypeStruct(initial_field.shape, jnp.float32),
        in_specs=[vmem] * 3,
        out_specs=vmem,
        scratch_shapes=[
            pltpu.VMEM((2, halves, count, block, LANES), jnp.float32),
            pltpu.VMEM((2, halves, count * block, LANES), jnp.float32),
            pltpu.VMEM((halves, count * block, LANES), jnp.float32),
            pltpu.VMEM((halves, count, block, LANES), jnp.float32),
        ]
        + [spectral] * 9
        + [
            pltpu.SemaphoreType.DMA((5, halves)),
            pltpu.SemaphoreType.DMA((5, halves)),
            pltpu.SemaphoreType.DMA((4, halves)),
            pltpu.SemaphoreType.DMA((4, rows_x)),
        ],
        compiler_params=pltpu.CompilerParams(
            collective_id=0, has_side_effects=True, vmem_limit_bytes=60 * 1024 * 1024
        ),
    )(initial_field, jnp.asarray(left), jnp.asarray(right))


def solution(mesh):
    placed = (P(("row", "col"), None, None),)
    return jax.shard_map(
        body, mesh=mesh, in_specs=placed, out_specs=P(("row", "col"), None, None), check_vma=False
    )
```

```python
import functools
import math

import jax
import jax.numpy as jnp
import numpy as np
from jax import lax
from jax.experimental import pallas as pl
from jax.experimental.pallas import tpu as pltpu
from jax.sharding import PartitionSpec as P

growth_rate = 0.3
quadratic = 1.0
time_step = 0.2
wave_scale = 4.0


def wavenumbers(count, offset, length):
    indices = offset + jnp.arange(count)
    signed = jnp.where(indices * 2 < length, indices, indices - length)
    return wave_scale * signed.astype(jnp.float32) / length


def phi_values(argument):
    within = jnp.abs(argument) < 1.0
    inside = jnp.where(within, argument, 0.0)
    outside = jnp.where(within, 2.0, argument)
    series = []
    for degree in (1, 2, 3):
        running = jnp.zeros_like(argument) + 1.0 / math.factorial(11 + degree)
        for exponent in range(10, -1, -1):
            running = running * inside + 1.0 / math.factorial(exponent + degree)
        series.append(running)
    growth_term = jnp.exp(outside)
    closed_one = (growth_term - 1.0) / outside
    closed_two = (growth_term - 1.0 - outside) / (outside * outside)
    closed_three = (growth_term - 1.0 - outside - 0.5 * outside * outside) / (
        outside * outside * outside
    )
    return (
        jnp.where(within, series[0], closed_one),
        jnp.where(within, series[1], closed_two),
        jnp.where(within, series[2], closed_three),
    )


def step_factors(ksq):
    lin = growth_rate - (1.0 - ksq) * (1.0 - ksq)
    scaled = time_step * lin
    half_phi, _, _ = phi_values(0.5 * scaled)
    first_phi, second_phi, third_phi = phi_values(scaled)
    e_half = jnp.exp(0.5 * scaled)
    q_half = 0.5 * time_step * half_phi
    e_full = jnp.exp(scaled)
    f_one = time_step * (first_phi - 3.0 * second_phi + 4.0 * third_phi)
    f_two = time_step * (second_phi - 2.0 * third_phi)
    f_three = time_step * (4.0 * third_phi - second_phi)
    return (e_half, q_half, e_full, f_one, f_two, f_three)


def reaction(values):
    return quadratic * values * values - values * values * values


def cas_table(length):
    modes = jnp.arange(length, dtype=jnp.int32)
    product = jnp.mod(modes[:, None] * modes[None, :], length)
    angle = 2.0 * math.pi / length * product.astype(jnp.float32)
    return (jnp.cos(angle) + jnp.sin(angle)) / math.sqrt(length)


def contract(form, left, right):
    return jnp.einsum(
        form, left, right, precision=lax.Precision.HIGHEST, preferred_element_type=jnp.float32
    )


def move(blocks):
    return lax.all_to_all(blocks, ("row", "col"), split_axis=0, concat_axis=0, tiled=True)


def plain_body(initial_field):
    devices_all = lax.axis_size("row") * lax.axis_size("col")
    rows_x, size_y, size_z = initial_field.shape
    size_x = rows_x * devices_all
    share_y = size_y // devices_all
    table_z = cas_table(size_z)
    table_y = cas_table(size_y).reshape((devices_all, share_y, size_y))
    table_x = cas_table(size_x).reshape((devices_all, rows_x, size_x))
    offset = lax.axis_index(("row", "col")) * share_y
    wave_y = wavenumbers(share_y, offset, size_y)
    wave_z = wavenumbers(size_z, 0, size_z)
    wave_x = wavenumbers(size_x, 0, size_x)
    ksq = wave_y[:, None, None] ** 2 + wave_z[None, None, :] ** 2 + wave_x[None, :, None] ** 2
    e_half, q_half, e_full, f_one, f_two, f_three = step_factors(ksq)

    def forward_all(values):
        over_z = contract("xyn,nk->xyk", values, table_z)
        over_y = contract("sly,xyk->slxk", table_y, over_z)
        return contract("sxX,slxk->lXk", table_x, move(over_y))

    def inverse_all(spectra):
        over_x = contract("sxX,lXk->slxk", table_x, spectra)
        over_y = contract("slxk,sly->xyk", move(over_x), table_y)
        return contract("xyk,kn->xyn", over_y, table_z)

    def react_spectrum(spectrum):
        return forward_all(reaction(inverse_all(spectrum)))

    state_hat = forward_all(initial_field)
    react_u = forward_all(reaction(initial_field))
    first_hat = e_half * state_hat + q_half * react_u
    react_a = react_spectrum(first_hat)
    second_hat = e_half * state_hat + q_half * react_a
    react_b = react_spectrum(second_hat)
    third_hat = e_half * first_hat + q_half * (2.0 * react_b - react_u)
    react_c = react_spectrum(third_hat)
    new_hat = (
        e_full * state_hat + f_one * react_u + 2.0 * f_two * (react_a + react_b) + f_three * react_c
    )
    return inverse_all(new_hat)


LANES = 128


def split_table(length):
    modes = np.arange(length)
    angle = 2.0 * np.pi / length * ((modes[:, None] * modes[None, :]) % length)
    table = ((np.cos(angle) + np.sin(angle)) / np.sqrt(length)).astype(np.float32)
    upper = table.astype(jnp.bfloat16)
    lower = (table - upper.astype(np.float32)).astype(jnp.bfloat16)
    return upper, lower


def split_values(values):
    upper = values.astype(jnp.bfloat16)
    lower = (values - upper.astype(jnp.float32)).astype(jnp.bfloat16)
    return upper, lower


def kernel(
    count, columns, rows_x, share_y, size_x, size_y, size_z,
    field_in, left, right, out_to,
    send_f, got_f, send_i, got_i, held, third, total,
    e_half, q_half, e_full, f_one, f_two, f_three,
    sent_f, came_f, sent_i, came_i, field, out, plane_in, plane_out,
):
    me = lax.axis_index("row") * columns + lax.axis_index("col")
    block = rows_x * share_y
    halves = size_z // LANES
    pairs = share_y // 2
    group = 1
    parts = rows_x // group
    early = parts // 2

    def mul_left(values):
        upper, lower = split_values(values)
        stacked = jnp.concatenate([upper, lower, upper], axis=0)
        return jnp.dot(left[...], stacked, preferred_element_type=jnp.float32)

    def mul_right(values):
        upper, lower = split_values(values)
        stacked = jnp.concatenate([upper, lower, upper], axis=1)
        return jnp.dot(stacked, right[...], preferred_element_type=jnp.float32)

    def load(m):
        return pltpu.make_async_copy(field_in.at[m], field.at[m], plane_in.at[m])

    def store(m):
        return pltpu.make_async_copy(out.at[m], out_to.at[m], plane_out.at[m])

    for m in range(rows_x):
        load(m).start()
    barrier = pltpu.get_barrier_semaphore()

    def greet(offset, carry):
        other = (me + offset) % count
        pl.semaphore_signal(
            barrier,
            inc=1,
            device_id=(other // columns, other % columns),
            device_id_type=pl.DeviceIdType.MESH,
        )
        return carry

    lax.fori_loop(1, count, greet, 0)

    def send_forward(index, half, start, length):
        buffer = index % 2
        here = pl.multiple_of(me * block + start, 8)
        mine = got_f.at[buffer, half, pl.ds(here, length), :]
        pltpu.make_async_copy(
            send_f.at[buffer, half, me, pl.ds(start, length), :], mine, came_f.at[index, half]
        ).start()

        def one(offset, carry):
            other = (me + offset) % count
            pltpu.make_async_remote_copy(
                src_ref=send_f.at[buffer, half, other, pl.ds(start, length), :],
                dst_ref=mine,
                send_sem=sent_f.at[index, half],
                recv_sem=came_f.at[index, half],
                device_id=(other // columns, other % columns),
                device_id_type=pl.DeviceIdType.MESH,
            ).start()
            return carry

        lax.fori_loop(1, count, one, 0)

    def send_inverse(index, half, part):
        length = group * share_y
        mine = got_i.at[half, me, pl.ds(part * length, length), :]

        def rows(device):
            start = pl.multiple_of(device * block + part * length, 8)
            return send_i.at[half, pl.ds(start, length), :]

        pltpu.make_async_copy(rows(me), mine, came_i.at[index, part]).start()

        def one(offset, carry):
            other = (me + offset) % count
            pltpu.make_async_remote_copy(
                src_ref=rows(other),
                dst_ref=mine,
                send_sem=sent_i.at[index, half],
                recv_sem=came_i.at[index, part],
                device_id=(other // columns, other % columns),
                device_id_type=pl.DeviceIdType.MESH,
            ).start()
            return carry

        lax.fori_loop(1, count, one, 0)

    def wait_bytes(ref, sem):
        pltpu.make_async_copy(ref, ref, sem).wait()

    def wait_sent_forward(index):
        for half in range(halves):
            wait_bytes(send_f.at[index % 2, half, pl.ds(0, count - 1)], sent_f.at[index, half])

    def wait_sent_inverse(index, half):
        wait_bytes(send_i.at[half, pl.ds(0, (count - 1) * block), :], sent_i.at[index, half])

    def forward(index, source, before=None):
        def plane(m):
            spectrum = mul_left(mul_right(source(m)))
            rows = pl.ds(pl.multiple_of(m * share_y, 8), share_y)
            for half in range(halves):
                part = spectrum[:, half * LANES : (half + 1) * LANES]
                send_f[index % 2, half, :, rows, :] = part.reshape(count, share_y, LANES)

        def step(g, carry):
            if before is not None:
                before(g)
            for inner in range(group):
                plane(g * group + inner)
            send_forward(
                index, 0, pl.multiple_of(g * group * share_y, 8), group * share_y
            )
            return carry

        first = 0
        if index == 0:
            for m in range(group):
                load(m).wait()
                plane(m)
            pl.semaphore_wait(barrier, count - 1)
            send_forward(0, 0, 0, group * share_y)
            first = 1
        lax.fori_loop(first, parts, step, 0)
        for half in range(1, halves):
            send_forward(index, half, 0, block)

    def physical(m):
        rows = pl.ds(pl.multiple_of(m * share_y, 8), share_y)
        parts = [got_i[half, :, rows, :].reshape(size_y, LANES) for half in range(halves)]
        return mul_right(mul_left(jnp.concatenate(parts, axis=1)))

    def spectrum_at(index, half, pair):
        parts = [
            got_f[index % 2, half, pl.ds(pair * 2 + inner, size_x, stride=share_y), :]
            for inner in range(2)
        ]
        return mul_left(jnp.concatenate(parts, axis=1))

    def arrived_forward(index, half):
        wait_bytes(got_f.at[index % 2, half], came_f.at[index, half])

    def inverse(index, source, update):
        for half in range(halves):
            arrived_forward(source, half)
            if index > 0:
                wait_sent_inverse(index - 1, half)

            def step(pair, carry):
                values = mul_left(update(half, pair, spectrum_at(source, half, pair)))
                for inner in range(2):
                    send_i[half, pl.ds(pair * 2 + inner, size_x, stride=share_y), :] = values[
                        :, inner * LANES : (inner + 1) * LANES
                    ]
                return carry

            lax.fori_loop(0, pairs, step, 0)
            for part in range(early):
                send_inverse(index, half, part)
        for part in range(early, parts):
            for half in range(halves):
                send_inverse(index, half, part)

    def arrived_inverse(index, part):
        length = group * share_y
        rows = pl.ds(pl.multiple_of(part * length, 8), length)
        wait_bytes(got_i.at[:, :, rows, :], came_i.at[index, part])

    def wave(indices, length):
        signed = jnp.where(indices * 2 < length, indices, indices - length)
        return wave_scale * signed.astype(jnp.float32) / length

    def loaded(g):
        for inner in range(group):
            load(g * group + inner).wait()

    forward(0, lambda m: field[m], loaded)
    forward(1, lambda m: reaction(field[m]))

    rows_step = 32

    def factors(item, carry):
        half = item // (pairs * (size_x // rows_step))
        rest = item % (pairs * (size_x // rows_step))
        pair = rest // (size_x // rows_step)
        start = pl.multiple_of(rest % (size_x // rows_step) * rows_step, 8)
        dims = (rows_step, 2 * LANES)
        lane = lax.broadcasted_iota(jnp.int32, dims, 1)
        second = (lane >= LANES).astype(jnp.int32)
        index_z = lane - second * LANES + half * LANES
        index_y = second + (me * share_y + pair * 2)
        index_x = lax.broadcasted_iota(jnp.int32, dims, 0) + start
        wave_y, wave_z, wave_x = wave(index_y, size_y), wave(index_z, size_z), wave(index_x, size_x)
        ksq = wave_y * wave_y + wave_z * wave_z + wave_x * wave_x
        values = step_factors(ksq)
        where = pl.ds(start, rows_step)
        for ref, value in zip((e_half, q_half, e_full, f_one, f_two, f_three), values):
            ref[half, pair, where, :] = value
        return carry

    lax.fori_loop(0, halves * pairs * (size_x // rows_step), factors, 0)

    for half in range(halves):
        arrived_forward(0, half)

        def keep(pair, carry):
            total[half, pair] = spectrum_at(0, half, pair)
            return carry

        lax.fori_loop(0, pairs, keep, 0)

    def update_first(half, pair, react_u):
        state_hat = total[half, pair]
        base = e_half[half, pair] * state_hat
        gain = q_half[half, pair] * react_u
        first_hat = base + gain
        held[half, pair] = base
        third[half, pair] = e_half[half, pair] * first_hat - gain
        total[half, pair] = e_full[half, pair] * state_hat + f_one[half, pair] * react_u
        return first_hat

    def update_second(half, pair, react_a):
        total[half, pair] = total[half, pair] + 2.0 * f_two[half, pair] * react_a
        return held[half, pair] + q_half[half, pair] * react_a

    def update_third(half, pair, react_b):
        total[half, pair] = total[half, pair] + 2.0 * f_two[half, pair] * react_b
        return third[half, pair] + 2.0 * q_half[half, pair] * react_b

    def update_last(half, pair, react_c):
        return total[half, pair] + f_three[half, pair] * react_c

    updates = (update_first, update_second, update_third, update_last)
    for index, update in enumerate(updates):
        inverse(index, index + 1, update)
        if index < 3:
            wait_sent_forward(index)
            forward(
                index + 2,
                lambda m: reaction(physical(m)),
                lambda g, index=index: arrived_inverse(index, g),
            )
    for index in (3, 4):
        wait_sent_forward(index)

    def finish(g, carry):
        arrived_inverse(3, g)
        for inner in range(group):
            out[g * group + inner] = physical(g * group + inner)
            store(g * group + inner).start()
        return carry

    lax.fori_loop(0, parts, finish, 0)
    for half in range(halves):
        wait_sent_inverse(3, half)
    for m in range(rows_x):
        store(m).wait()


def body(initial_field):
    rows_x, size_y, size_z = initial_field.shape
    columns = lax.axis_size("col")
    count = lax.axis_size("row") * columns
    size_x = rows_x * count
    share_y = size_y // count
    fits = share_y % 8 == 0 and size_z % LANES == 0 and size_x == size_y == size_z
    if not fits:
        return plain_body(initial_field)
    upper, lower = split_table(size_x)
    left = np.concatenate([upper, upper, lower], axis=1)
    right = np.concatenate([upper, upper, lower], axis=0)
    halves, pairs, block = size_z // LANES, share_y // 2, rows_x * share_y
    spectral = pltpu.VMEM((halves, pairs, size_x, 2 * LANES), jnp.float32)
    vmem = pl.BlockSpec(memory_space=pltpu.VMEM)
    return pl.pallas_call(
        functools.partial(
            kernel, count, columns, rows_x, share_y, size_x, size_y, size_z
        ),
        out_shape=jax.ShapeDtypeStruct(initial_field.shape, jnp.float32),
        in_specs=[pl.BlockSpec(memory_space=pltpu.HBM), vmem, vmem],
        out_specs=pl.BlockSpec(memory_space=pltpu.HBM),
        scratch_shapes=[
            pltpu.VMEM((2, halves, count, block, LANES), jnp.float32),
            pltpu.VMEM((2, halves, count * block, LANES), jnp.float32),
            pltpu.VMEM((halves, count * block, LANES), jnp.float32),
            pltpu.VMEM((halves, count, block, LANES), jnp.float32),
        ]
        + [spectral] * 9
        + [
            pltpu.SemaphoreType.DMA((5, halves)),
            pltpu.SemaphoreType.DMA((5, halves)),
            pltpu.SemaphoreType.DMA((4, halves)),
            pltpu.SemaphoreType.DMA((4, rows_x)),
            pltpu.VMEM(initial_field.shape, jnp.float32),
            pltpu.VMEM(initial_field.shape, jnp.float32),
            pltpu.SemaphoreType.DMA((rows_x,)),
            pltpu.SemaphoreType.DMA((rows_x,)),
        ],
        compiler_params=pltpu.CompilerParams(
            collective_id=0, has_side_effects=True, vmem_limit_bytes=60 * 1024 * 1024
        ),
    )(initial_field, jnp.asarray(left), jnp.asarray(right))


def solution(mesh):
    placed = (P(("row", "col"), None, None),)
    return jax.shard_map(
        body, mesh=mesh, in_specs=placed, out_specs=P(("row", "col"), None, None), check_vma=False
    )
```
